512 devices in a mesh: row: 32 (over z, y_hi), col: 16 (over y_lo, x, core).
Axes of the slice: x: 4, y: 4 (y_hi: 2, y_lo: 2; y = y_hi * 2 + y_lo), z: 16, core: 2. Of those that a mesh axis runs over, the one named last changes fastest.
Arguments:
- image_embed: float32 [65536, 1152], P(('row', 'col')), may hold values from -150 to 150, as said below
- text_embed: float32 [65536, 1152], P(('row', 'col')), may hold values from -150 to 150
- log_scale: float32 [1], replicated, may hold values from 1.8 to 2.6
- bias: float32 [1], replicated, may hold values from -6 to -3
Outputs:
- loss: float32 [1], replicated
- image_grad: float32 [65536, 1152], P(('row', 'col'))
- text_grad: float32 [65536, 1152], P(('row', 'col'))
The draws below stay inside these ranges and needn't reach their ends.
Inputs may be any that keep to these rules, and one draw needn't show every extreme that they name: Row i of image_embed and row i of text_embed are correlated.
All inputs are finite; a program needn't handle non-finite values.
Results may differ from the reference program's by a relative error of at most 0.0046.
Values may be sent and summed in bfloat16 or wider, within the bound.
A program may use at most 64 MiB of HBM per device.

```python
import math
import jax
import jax.numpy as jnp
from jax import lax

D = 1152
GROUP = 2048
TOTAL = 65536
N_ROW = 32


def pair_draw(key):
    keys = jax.random.split(jax.random.fold_in(key, 7), 6)
    base = jnp.clip(jax.random.normal(keys[0], (TOTAL, D), jnp.float32), -4.0, 4.0)
    noise_img = jnp.clip(jax.random.normal(keys[1], (TOTAL, D), jnp.float32), -4.0, 4.0)
    noise_txt = jnp.clip(jax.random.normal(keys[2], (TOTAL, D), jnp.float32), -4.0, 4.0)
    column = jnp.exp(jax.random.uniform(keys[3], (1, D), jnp.float32, 0.0, math.log(10.0)))
    row_img = jnp.exp(jax.random.uniform(keys[4], (TOTAL, 1), jnp.float32, 0.0, math.log(10.0)))
    row_txt = jnp.exp(jax.random.uniform(keys[5], (TOTAL, 1), jnp.float32, 0.0, math.log(10.0)))
    divisor = jnp.sqrt(jnp.float32(D))
    image = (base + 0.8 * noise_img) * column * row_img / divisor
    text = (0.7 * base + noise_txt) * column * row_txt / divisor
    return (image, text)


def draw_image_embed(key, part):
    return pair_draw(key)[0]


def draw_text_embed(key, part):
    return pair_draw(key)[1]


def setup_inputs(seed: int = 0) -> dict:
    splits = jax.random.split(jax.random.key(seed), 5)
    return {
        "image_embed": draw_image_embed(jax.random.fold_in(splits[4], 71), 0),
        "text_embed": draw_text_embed(jax.random.fold_in(splits[4], 71), 0),
        "log_scale": jnp.clip(jax.random.uniform(splits[2], (1,), jnp.float32, 1.8, 2.6), 1.8, 2.6),
        "bias": jnp.clip(jax.random.uniform(splits[3], (1,), jnp.float32, -6.0, -3.0), -6.0, -3.0),
    }


def unit_rows(values):
    inverse = 1.0 / jnp.sqrt(lax.optimization_barrier(jnp.sum(values * values, axis=1, keepdims=True)) + 1e-06)
    return (values * inverse, inverse)

def back_rows(grad_unit, unit, inverse):
    return inverse * (grad_unit - lax.optimization_barrier(jnp.sum(grad_unit * unit, axis=1, keepdims=True)) * unit)

def reference(image_embed, text_embed, log_scale, bias):
    scale = jnp.exp(log_scale[0])
    offset = bias[0]

    def one_batch(pair):
        images, texts = pair
        img_unit, img_inv = unit_rows(images)
        txt_unit, txt_inv = unit_rows(texts)
        img_b = img_unit.astype(jnp.bfloat16)
        txt_b = txt_unit.astype(jnp.bfloat16)
        logits = scale * jnp.dot(img_b, txt_b.T, preferred_element_type=jnp.float32) + offset
        index = jnp.arange(GROUP, dtype=jnp.int32)
        sign = jnp.where(index[:, None] == index[None, :], 1.0, -1.0).astype(logits.dtype)
        total = jnp.sum(jax.nn.softplus(-sign * logits))
        weight = (-sign * jax.nn.sigmoid(-sign * logits)).astype(jnp.bfloat16)
        img_gu = scale * jnp.dot(weight, txt_b, preferred_element_type=jnp.float32)
        txt_gu = scale * jnp.dot(weight.T, img_b, preferred_element_type=jnp.float32)
        return (total, back_rows(img_gu, img_unit, img_inv), back_rows(txt_gu, txt_unit, txt_inv))
    images = image_embed.reshape(N_ROW, GROUP, D)
    texts = text_embed.reshape(N_ROW, GROUP, D)
    totals, image_grad, text_grad = lax.map(one_batch, (images, texts))
    loss = (jnp.sum(totals) / TOTAL).reshape(1)
    return (loss, image_grad.reshape(TOTAL, D), text_grad.reshape(TOTAL, D))
```

```python
import functools

import jax
import jax.numpy as jnp
from jax import lax
from jax.experimental import pallas as pl
from jax.experimental.pallas import tpu as pltpu
from jax.sharding import Mesh
from jax.sharding import PartitionSpec as P

AXES = ("z", "yh", "yl", "x", "c")
MESH = pl.DeviceIdType.MESH
BF = jnp.bfloat16
F32 = jnp.float32
CHUNK = 384


def nt_dot(a, b):
    return lax.dot_general(a, b, (((1,), (1,)), ((), ())), preferred_element_type=F32)


def tn_dot(a, b):
    return lax.dot_general(a, b, (((0,), (0,)), ((), ())), preferred_element_type=F32)


def kernel(
    log_scale_ref, bias_ref, img_hbm, txt_hbm,
    loss_ref, img_grad, txt_grad,
    img_x, txt_x, img_inv, txt_inv, img_all, txt_all, logit, weight,
    own_p, hold_p, own_q, hold_q,
    out_right, out_left, out_opp, out_sib, out_diag, out_comb, out_part,
    way_x, fin_left, fin_right, way_t, fin_sib, fin_part,
    loss_box, loss_out, loss_in1, loss_in2, loss_in3,
    load_sem, send_sem, recv_sem, lsend_sem, lrecv_sem, near_sem,
):
    rows, width = img_x.shape
    half = rows // 2
    nz, nyh, nx = lax.axis_size("z"), lax.axis_size("yh"), lax.axis_size("x")
    ny = 2 * nyh
    z, yh, yl = lax.axis_index("z"), lax.axis_index("yh"), lax.axis_index("yl")
    x, c = lax.axis_index("x"), lax.axis_index("c")
    y = yh * 2 + yl

    def at_x(step, core=0):
        return {"x": lax.rem(x + step, nx), "c": lax.rem(c + core, 2)}

    def at_y(step):
        there = lax.rem(y + step, ny)
        return {"yh": there // 2, "yl": lax.rem(there, 2)}

    def at_z(step):
        return {"z": lax.rem(z + step, nz)}

    right, left, sibling = at_x(1), at_x(nx - 1), at_x(0, 1)
    partner = {"yl": 1 - yl}

    load_img = pltpu.make_async_copy(img_hbm, img_x, load_sem.at[0])
    load_txt = pltpu.make_async_copy(txt_hbm, txt_x, load_sem.at[1])
    load_img.start()
    load_txt.start()

    around = [right, left, sibling, at_y(1), at_y(ny - 1), at_z(1), at_z(nz - 1)]
    barrier = pltpu.get_barrier_semaphore()
    for peer in around:
        pl.semaphore_signal(barrier, inc=1, device_id=peer, device_id_type=MESH)

    def send(index, source, target, peer):
        copy = pltpu.make_async_remote_copy(
            src_ref=source, dst_ref=target, send_sem=send_sem.at[index], recv_sem=recv_sem.at[index],
            device_id=peer, device_id_type=MESH,
        )
        copy.start()
        return copy

    def normalize(values, inverse, packed):
        step = 32
        for start in range(0, rows, step):
            part = values[start : start + step, :]
            inv = lax.rsqrt(jnp.sum(part * part, axis=1, keepdims=True) + 1e-06)
            inverse[start : start + step, :] = inv
            packed[start : start + step, :] = (part * inv).astype(BF)

    a, b = pl.ds(0, half), pl.ds(half, half)

    def slot(index, offset=0, size=None):
        return pl.ds(index * rows + offset, rows if size is None else size)

    load_img.wait()
    normalize(img_x, img_inv, img_all)
    pl.semaphore_wait(barrier, len(around))
    right_a = send(0, img_all.at[a], img_all.at[slot(1, 0, half)], right)
    left_b = send(2, img_all.at[b], img_all.at[slot(2, half, half)], left)
    right_b = send(1, img_all.at[b], img_all.at[slot(1, half, half)], right)
    left_a = send(3, img_all.at[a], img_all.at[slot(2, 0, half)], left)
    load_txt.wait()
    normalize(txt_x, txt_inv, txt_all)
    txt_part = send(7, txt_all.at[slot(0)], txt_all.at[slot(2)], partner)
    txt_sib = send(6, txt_all.at[slot(0)], txt_all.at[slot(1)], sibling)

    for index, group in enumerate((around, [at_z(2), at_z(nz - 2), sibling], [at_z(4), at_z(nz - 4)])):
        for peer in group:
            pl.semaphore_signal(near_sem.at[index], inc=1, device_id=peer, device_id_type=MESH)
        pl.semaphore_wait(near_sem.at[index], len(group))

    right_a.wait_recv()
    pass_right = send(4, img_all.at[slot(1, 0, half)], img_all.at[slot(3, 0, half)], right)
    left_b.wait_recv()
    pass_left = send(5, img_all.at[slot(2, half, half)], img_all.at[slot(3, half, half)], left)
    txt_part.wait_recv()
    txt_diag = send(8, txt_all.at[slot(2)], txt_all.at[slot(3)], sibling)

    log_scale = jnp.full((1, 4 * rows), log_scale_ref[0], F32)
    scale = jnp.exp(log_scale)
    offset = jnp.full((1, 4 * rows), bias_ref[0], F32)

    def weights(index):
        logits = scale * nt_dot(img_all[slot(index), :], txt_all[...]) + offset
        logit[slot(index), :] = logits
        small = jnp.exp(-jnp.abs(logits))
        inv = 1.0 / (1.0 + small)
        value = jnp.where(logits >= 0, 1.0, small) * inv
        if index == 0:
            mine = (lax.broadcasted_iota(jnp.int32, value.shape, 0)
                    == lax.broadcasted_iota(jnp.int32, value.shape, 1))
            value = jnp.where(mine, -jnp.where(logits >= 0, small, 1.0) * inv, value)
        weight[slot(index), :] = value.astype(BF)

    def img_term(index, start):
        return jnp.dot(weight[slot(index), :], txt_all[:, start : start + CHUNK], preferred_element_type=F32)

    def txt_term(index, start):
        block = weight[:, index * rows : (index + 1) * rows]
        return tn_dot(block, img_all[:, start : start + CHUNK])

    chunks = [(start, slice(start, start + CHUNK)) for start in range(0, width, CHUNK)]

    txt_sib.wait_recv()
    txt_diag.wait_recv()
    weights(0)
    right_b.wait_recv()
    left_a.wait_recv()
    weights(1)
    weights(2)
    for start, cols in chunks:
        term = img_term(2, start)
        hold_p[0:half, cols] = term[0:half]
        out_right[:, cols] = term[half:].astype(BF)
    to_right = send(11, out_right, fin_left.at[b], right)
    for start, cols in chunks:
        term = img_term(1, start)
        hold_p[half:, cols] = term[half:]
        out_left[:, cols] = term[0:half].astype(BF)
    to_left = send(12, out_left, fin_right.at[a], left)
    for start, cols in chunks:
        own_p[:, cols] = img_term(0, start)

    pass_right.wait_recv()
    pass_left.wait_recv()
    weights(3)
    for start, cols in chunks:
        out_opp[:, cols] = img_term(3, start).astype(BF)
    opp_right = send(9, out_opp.at[a], way_x.at[a], right)
    opp_left = send(10, out_opp.at[b], way_x.at[b], left)
    for start, cols in chunks:
        out_diag[:, cols] = txt_term(3, start).astype(BF)
    diag = send(15, out_diag, way_t, sibling)
    for start, cols in chunks:
        out_sib[:, cols] = txt_term(1, start).astype(BF)
    sib = send(16, out_sib, fin_sib, sibling)
    for start, cols in chunks:
        hold_q[:, cols] = txt_term(2, start)
    for start, cols in chunks:
        own_q[:, cols] = txt_term(0, start)

    total = jnp.zeros((8, 4 * rows), F32)
    step = 64
    for start in range(0, 4 * rows, step):
        logits = logit[start : start + step, :]
        flip = jnp.maximum(logits, 0.0)
        if start < rows:
            mine = (lax.broadcasted_iota(jnp.int32, logits.shape, 0) + start
                    == lax.broadcasted_iota(jnp.int32, logits.shape, 1))
            flip = jnp.where(mine, jnp.maximum(-logits, 0.0), flip)
        terms = flip + jnp.log1p(jnp.exp(-jnp.abs(logits)))
        total = total + jnp.sum(terms.reshape(step // 8, 8, 4 * rows), axis=0)
    total = jnp.sum(total, axis=0, keepdims=True)
    total = sum(total[:, k * rows : (k + 1) * rows] for k in range(4))

    lsent = []

    def spread(base, value, stage, inbox, peers):
        loss_out[stage] = value
        copies = []
        for k, peer in enumerate(peers):
            copy = pltpu.make_async_remote_copy(
                src_ref=loss_out.at[stage], dst_ref=inbox.at[k], send_sem=lsend_sem.at[base + k],
                recv_sem=lrecv_sem.at[base + k], device_id=peer, device_id_type=MESH,
            )
            copy.start()
            copies.append(copy)
        lsent.extend(copies)
        return copies

    def gather(value, copies, inbox):
        for k, copy in enumerate(copies):
            copy.wait_recv()
            value = value + inbox[k]
        return value

    plane = [at_x(step, core) for core in range(2) for step in range(nx) if step or core]
    first = spread(0, total, 0, loss_in1, plane)

    diag.wait_recv()
    for start, cols in chunks:
        out_part[:, cols] = (hold_q[:, cols] + way_t[:, cols].astype(F32)).astype(BF)
    part = send(17, out_part, fin_part, partner)

    total = gather(total, first, loss_in1)
    second = spread(len(plane), total, 1, loss_in2, [at_y(step) for step in range(1, ny)])

    opp_right.wait_recv()
    out_comb[a] = (hold_p[a] + way_x[a].astype(F32)).astype(BF)
    comb_right = send(13, out_comb.at[a], fin_left.at[a], right)
    opp_left.wait_recv()
    out_comb[b] = (hold_p[b] + way_x[b].astype(F32)).astype(BF)
    comb_left = send(14, out_comb.at[b], fin_right.at[b], left)

    total = gather(total, second, loss_in2)
    third = spread(len(plane) + ny - 1, total, 2, loss_in3, [at_z(step) for step in range(1, nz)])

    scale = jnp.exp(jnp.full((1, width), log_scale_ref[0], F32))

    def back(own, one, two, values, inverse, target):
        step = 32
        for start in range(0, rows, step):
            r = slice(start, start + step)
            grad = scale * (own[r, :] + one[r, :].astype(F32) + two[r, :].astype(F32))
            inv = inverse[r, :]
            unit = values[r, :] * inv
            target[r, :] = inv * (grad - jnp.sum(grad * unit, axis=1, keepdims=True) * unit)

    to_right.wait_recv()
    to_left.wait_recv()
    sib.wait_recv()
    part.wait_recv()
    back(own_q, fin_sib, fin_part, txt_x, txt_inv, txt_grad)
    comb_right.wait_recv()
    comb_left.wait_recv()
    back(own_p, fin_left, fin_right, img_x, img_inv, img_grad)

    total = gather(total, third, loss_in3)
    count = rows * 4 * nx * nyh * nz
    loss_ref[0] = jnp.sum(total) * (1.0 / count)

    for copy in (
        right_a, left_b, right_b, left_a, txt_part, txt_sib, pass_right, pass_left, txt_diag, to_right, to_left,
        opp_right, opp_left, diag, sib, part, comb_right, comb_left, *lsent,
    ):
        copy.wait_send()


def local(image_embed, text_embed, log_scale, bias):
    rows, width = image_embed.shape
    half = rows // 2
    nx, ny, nz = lax.axis_size("x"), 2 * lax.axis_size("yh"), lax.axis_size("z")
    peers = 2 * nx - 1 + ny - 1 + nz - 1
    smem = pl.BlockSpec(memory_space=pltpu.SMEM)
    hbm = pl.BlockSpec(memory_space=pltpu.HBM)
    vmem = pl.BlockSpec(memory_space=pltpu.VMEM)
    block = pltpu.VMEM((rows, width), BF)
    wide = pltpu.VMEM((rows, width), F32)
    part = pltpu.VMEM((half, width), BF)
    column = pltpu.VMEM((rows, 1), F32)
    return pl.pallas_call(
        kernel,
        out_shape=(
            jax.ShapeDtypeStruct((1,), F32),
            jax.ShapeDtypeStruct((rows, width), F32),
            jax.ShapeDtypeStruct((rows, width), F32),
        ),
        in_specs=[smem, smem, hbm, hbm],
        out_specs=(smem, vmem, vmem),
        scratch_shapes=[
            wide, wide, column, column,
            pltpu.VMEM((4 * rows, width), BF), pltpu.VMEM((4 * rows, width), BF),
            pltpu.VMEM((4 * rows, 4 * rows), F32), pltpu.VMEM((4 * rows, 4 * rows), BF),
            wide, wide, wide, wide,
            part, part, block, block, block, block, block,
            block, block, block, block, block, block,
            pltpu.VMEM((1, 128), F32), pltpu.VMEM((3, 1, 128), F32),
            pltpu.VMEM((2 * nx - 1, 1, 128), F32), pltpu.VMEM((ny - 1, 1, 128), F32),
            pltpu.VMEM((max(nz - 1, 1), 1, 128), F32),
            pltpu.SemaphoreType.DMA((2,)), pltpu.SemaphoreType.DMA((18,)), pltpu.SemaphoreType.DMA((18,)),
            pltpu.SemaphoreType.DMA((peers,)), pltpu.SemaphoreType.DMA((peers,)),
            pltpu.SemaphoreType.REGULAR((3,)),
        ],
        compiler_params=pltpu.CompilerParams(
            collective_id=0, has_side_effects=True, vmem_limit_bytes=48 * 1024 * 1024
        ),
        name="siglip",
    )(log_scale, bias, image_embed, text_embed)


def solution(mesh):
    split = Mesh(mesh.devices.reshape(16, 2, 2, 4, 2), AXES)
    rows = P(AXES, None)
    return jax.shard_map(
        local, mesh=split, in_specs=(rows, rows, P(), P()), out_specs=(P(), rows, rows), check_vma=False
    )
```

```python
import functools

import jax
import jax.numpy as jnp
from jax import lax
from jax.experimental import pallas as pl
from jax.experimental.pallas import tpu as pltpu
from jax.sharding import Mesh
from jax.sharding import PartitionSpec as P

AXES = ("z", "yh", "yl", "x", "c")
MESH = pl.DeviceIdType.MESH
BF = jnp.bfloat16
F32 = jnp.float32
CHUNK = 384


def in_hbm(value):
    return pltpu.with_memory_space_constraint(value, pltpu.HBM)


def nt_dot(a, b):
    return lax.dot_general(a, b, (((1,), (1,)), ((), ())), preferred_element_type=F32)


def tn_dot(a, b):
    return lax.dot_general(a, b, (((0,), (0,)), ((), ())), preferred_element_type=F32)


def kernel(
    log_scale_ref, bias_ref, img_hbm, txt_hbm,
    loss_ref, img_grad, txt_grad,
    img_x, txt_x, img_inv, txt_inv, img_all, txt_all, logit, weight,
    own_p, hold_p, own_q, hold_q,
    out_right, out_left, out_opp, out_sib, out_diag, out_comb, out_part,
    way_x, fin_left, fin_right, way_t, fin_sib, fin_part,
    loss_out, loss_in1, loss_in3,
    load_sem, send_sem, recv_sem, lsend_sem, lrecv_sem, near_sem,
):
    rows, width = img_x.shape
    half = rows // 2
    nz, nyh, nx = lax.axis_size("z"), lax.axis_size("yh"), lax.axis_size("x")
    ny = 2 * nyh
    z, yh, yl = lax.axis_index("z"), lax.axis_index("yh"), lax.axis_index("yl")
    x, c = lax.axis_index("x"), lax.axis_index("c")
    y = yh * 2 + yl

    def at_x(step, core=0):
        return {"x": lax.rem(x + step, nx), "c": lax.rem(c + core, 2)}

    def at_y(step):
        there = lax.rem(y + step, ny)
        return {"yh": there // 2, "yl": lax.rem(there, 2)}

    def at_z(step):
        return {"z": lax.rem(z + step, nz)}

    right, left, sibling = at_x(1), at_x(nx - 1), at_x(0, 1)
    partner = {"yl": 1 - yl}

    load_img = pltpu.make_async_copy(img_hbm, img_x, load_sem.at[0])
    load_txt = pltpu.make_async_copy(txt_hbm, txt_x, load_sem.at[1])
    load_img.start()
    load_txt.start()

    near = [right, left, sibling, at_y(1), at_y(ny - 1)]
    barrier = pltpu.get_barrier_semaphore()

    def signal(semaphore, peers):
        for peer in peers:
            pl.semaphore_signal(semaphore, inc=1, device_id=peer, device_id_type=MESH)

    def signal_if(condition, semaphore, peer):
        @pl.when(condition)
        def _():
            signal(semaphore, [peer])

    first_plane, last_plane = z == 0, z == nz - 1
    signal(barrier, near)
    signal_if(jnp.logical_not(last_plane), barrier, at_z(1))
    signal_if(first_plane, barrier, at_z(nz - 1))

    def send(index, source, target, peer):
        copy = pltpu.make_async_remote_copy(
            src_ref=source, dst_ref=target, send_sem=send_sem.at[index], recv_sem=recv_sem.at[index],
            device_id=peer, device_id_type=MESH,
        )
        copy.start()
        return copy

    def normalize(values, inverse, packed):
        step = 32
        for start in range(0, rows, step):
            part = values[start : start + step, :]
            inv = lax.rsqrt(jnp.sum(part * part, axis=1, keepdims=True) + 1e-06)
            inverse[start : start + step, :] = inv
            packed[start : start + step, :] = (part * inv).astype(BF)

    a, b = pl.ds(0, half), pl.ds(half, half)

    def slot(index, offset=0, size=None):
        return pl.ds(index * rows + offset, rows if size is None else size)

    load_img.wait()
    normalize(img_x, img_inv, img_all)
    pl.semaphore_wait(barrier, len(near) + jnp.where(first_plane, 0, 1) + jnp.where(last_plane, 1, 0))
    right_a = send(0, img_all.at[a], img_all.at[slot(1, 0, half)], right)
    left_b = send(2, img_all.at[b], img_all.at[slot(2, half, half)], left)
    right_b = send(1, img_all.at[b], img_all.at[slot(1, half, half)], right)
    left_a = send(3, img_all.at[a], img_all.at[slot(2, 0, half)], left)
    load_txt.wait()
    normalize(txt_x, txt_inv, txt_all)
    txt_part = send(7, txt_all.at[slot(0)], txt_all.at[slot(2)], partner)
    txt_sib = send(6, txt_all.at[slot(0)], txt_all.at[slot(1)], sibling)

    def round_of(index, peers):
        signal(near_sem.at[index], peers)

    round_of(0, near)
    signal_if(jnp.logical_not(first_plane), near_sem.at[0], at_z(nz - 1))
    signal_if(last_plane, near_sem.at[0], at_z(1))

    right_a.wait_recv()
    pass_right = send(4, img_all.at[slot(1, 0, half)], img_all.at[slot(3, 0, half)], right)
    left_b.wait_recv()
    pass_left = send(5, img_all.at[slot(2, half, half)], img_all.at[slot(3, half, half)], left)
    txt_part.wait_recv()
    txt_diag = send(8, txt_all.at[slot(2)], txt_all.at[slot(3)], sibling)
    pl.semaphore_wait(near_sem.at[0], len(near) + jnp.where(last_plane, 0, 1) + jnp.where(first_plane, 1, 0))
    round_of(1, [at_x(2), at_y(2), sibling, at_z(1), at_z(nz - 1)])

    log_scale = jnp.full((1, 4 * rows), log_scale_ref[0], F32)
    scale = jnp.exp(log_scale)
    offset = jnp.full((1, 4 * rows), bias_ref[0], F32)

    def diagonal(shape):
        return lax.broadcasted_iota(jnp.int32, shape, 0) == lax.broadcasted_iota(jnp.int32, shape, 1)

    def logits_of(index):
        logits = scale * nt_dot(img_all[slot(index), :], txt_all[...]) + offset
        logit[slot(index), :] = logits

    def loss_of(index):
        logits = logit[slot(index), :]
        flip = jnp.maximum(logits, 0.0)
        if index == 0:
            flip = jnp.where(diagonal(logits.shape), jnp.maximum(-logits, 0.0), flip)
        terms = flip + jnp.log1p(jnp.exp(-jnp.abs(logits)))
        return jnp.sum(terms.reshape(rows // 8, 8, 4 * rows), axis=0)

    def weights(index):
        logits = logit[slot(index), :]
        small = jnp.exp(-jnp.abs(logits))
        inv = 1.0 / (1.0 + small)
        value = jnp.where(logits >= 0, 1.0, small) * inv
        if index == 0:
            value = jnp.where(diagonal(value.shape), -jnp.where(logits >= 0, small, 1.0) * inv, value)
        weight[slot(index), :] = value.astype(BF)

    def img_term(index, start):
        return jnp.dot(weight[slot(index), :], txt_all[:, start : start + CHUNK], preferred_element_type=F32)

    def txt_term(index, start):
        block = weight[:, index * rows : (index + 1) * rows]
        return tn_dot(block, img_all[:, start : start + CHUNK])

    chunks = [(start, slice(start, start + CHUNK)) for start in range(0, width, CHUNK)]

    txt_sib.wait_recv()
    txt_diag.wait_recv()
    logits_of(0)
    total = loss_of(0)
    weights(0)
    right_b.wait_recv()
    left_a.wait_recv()
    for index in (1, 2):
        logits_of(index)
        total = total + loss_of(index)
        weights(index)
    pl.semaphore_wait(near_sem.at[1], 5)
    round_of(2, [sibling, at_z(2), at_z(nz - 2)])
    pass_right.wait_recv()
    pass_left.wait_recv()
    logits_of(3)
    total = jnp.sum(total + loss_of(3), axis=0, keepdims=True)
    total = sum(total[:, k * rows : (k + 1) * rows] for k in range(4))
    lsent = []

    def spread(base, value, stage, inbox, peers):
        loss_out[stage] = value
        copies = []
        for k, peer in enumerate(peers):
            copy = pltpu.make_async_remote_copy(
                src_ref=loss_out.at[stage], dst_ref=inbox.at[k], send_sem=lsend_sem.at[base + k],
                recv_sem=lrecv_sem.at[base + k], device_id=peer, device_id_type=MESH,
            )
            copy.start()
            copies.append(copy)
        lsent.extend(copies)
        return copies

    def gather(value, copies, inbox):
        for k, copy in enumerate(copies):
            copy.wait_recv()
            value = value + inbox[k]
        return value

    plane = [
        {**at_x(dx, dc), **at_y(dy)}
        for dy in range(ny) for dx in range(nx) for dc in range(2) if dy or dx or dc
    ]
    pl.semaphore_wait(near_sem.at[2], 3)
    round_of(3, [at_z(4), at_z(nz - 4)])
    first = spread(0, total, 0, loss_in1, plane)
    weights(3)
    for start, cols in chunks:
        term = img_term(2, start)
        hold_p[0:half, cols] = term[0:half]
        out_right[:, cols] = term[half:].astype(BF)
    to_right = send(11, out_right, fin_left.at[b], right)
    for start, cols in chunks:
        term = img_term(1, start)
        hold_p[half:, cols] = term[half:]
        out_left[:, cols] = term[0:half].astype(BF)
    to_left = send(12, out_left, fin_right.at[a], left)
    for start, cols in chunks:
        own_p[:, cols] = img_term(0, start)

    for start, cols in chunks:
        out_opp[:, cols] = img_term(3, start).astype(BF)
    opp_right = send(9, out_opp.at[a], way_x.at[a], right)
    opp_left = send(10, out_opp.at[b], way_x.at[b], left)
    for start, cols in chunks:
        out_diag[:, cols] = txt_term(3, start).astype(BF)
    diag = send(15, out_diag, way_t, sibling)
    for start, cols in chunks:
        out_sib[:, cols] = txt_term(1, start).astype(BF)
    sib = send(16, out_sib, fin_sib, sibling)
    for start, cols in chunks:
        hold_q[:, cols] = txt_term(2, start)
    for start, cols in chunks:
        own_q[:, cols] = txt_term(0, start)

    diag.wait_recv()
    for start, cols in chunks:
        out_part[:, cols] = (hold_q[:, cols] + way_t[:, cols].astype(F32)).astype(BF)
    part = send(17, out_part, fin_part, partner)

    total = gather(total, first, loss_in1)
    pl.semaphore_wait(near_sem.at[3], 2)
    third = spread(len(plane), total, 1, loss_in3, [at_z(step) for step in range(1, nz)])

    opp_right.wait_recv()
    out_comb[a] = (hold_p[a] + way_x[a].astype(F32)).astype(BF)
    comb_right = send(13, out_comb.at[a], fin_left.at[a], right)
    opp_left.wait_recv()
    out_comb[b] = (hold_p[b] + way_x[b].astype(F32)).astype(BF)
    comb_left = send(14, out_comb.at[b], fin_right.at[b], left)

    scale = jnp.exp(jnp.full((1, width), log_scale_ref[0], F32))

    def back(own, one, two, values, inverse, target):
        step = 32
        for start in range(0, rows, step):
            r = slice(start, start + step)
            grad = scale * (own[r, :] + one[r, :].astype(F32) + two[r, :].astype(F32))
            inv = inverse[r, :]
            unit = values[r, :] * inv
            target[r, :] = inv * (grad - jnp.sum(grad * unit, axis=1, keepdims=True) * unit)

    to_right.wait_recv()
    to_left.wait_recv()
    sib.wait_recv()
    part.wait_recv()
    back(own_q, fin_sib, fin_part, txt_x, txt_inv, txt_grad)
    comb_right.wait_recv()
    comb_left.wait_recv()
    back(own_p, fin_left, fin_right, img_x, img_inv, img_grad)

    total = gather(total, third, loss_in3)
    count = rows * 4 * nx * nyh * nz
    loss_ref[...] = total * (1.0 / count)

    for copy in (
        right_a, left_b, right_b, left_a, txt_part, txt_sib, pass_right, pass_left, txt_diag, to_right, to_left,
        opp_right, opp_left, diag, sib, part, comb_right, comb_left, *lsent,
    ):
        copy.wait_send()


def write(loss_row, img_grad, txt_grad, loss_ref, img_out, txt_out, sems):
    copies = [
        pltpu.make_async_copy(img_grad, img_out, sems.at[0]),
        pltpu.make_async_copy(txt_grad, txt_out, sems.at[1]),
    ]
    for copy in copies:
        copy.start()
    loss_ref[0] = jnp.sum(loss_row[...])
    for copy in copies:
        copy.wait()


def local(image_embed, text_embed, log_scale, bias):
    rows, width = image_embed.shape
    half = rows // 2
    nx, ny, nz = lax.axis_size("x"), 2 * lax.axis_size("yh"), lax.axis_size("z")
    plane = 2 * nx * ny - 1
    peers = plane + nz - 1
    smem = pl.BlockSpec(memory_space=pltpu.SMEM)
    hbm = pl.BlockSpec(memory_space=pltpu.HBM)
    vmem = pl.BlockSpec(memory_space=pltpu.VMEM)
    block = pltpu.VMEM((rows, width), BF)
    wide = pltpu.VMEM((rows, width), F32)
    part = pltpu.VMEM((half, width), BF)
    column = pltpu.VMEM((rows, 1), F32)
    loss_row, img_grad, txt_grad = pl.pallas_call(
        kernel,
        out_shape=(
            jax.ShapeDtypeStruct((1, 128), F32),
            jax.ShapeDtypeStruct((rows, width), F32),
            jax.ShapeDtypeStruct((rows, width), F32),
        ),
        in_specs=[smem, smem, hbm, hbm],
        out_specs=(vmem, vmem, vmem),
        scratch_shapes=[
            wide, wide, column, column,
            pltpu.VMEM((4 * rows, width), BF), pltpu.VMEM((4 * rows, width), BF),
            pltpu.VMEM((4 * rows, 4 * rows), F32), pltpu.VMEM((4 * rows, 4 * rows), BF),
            wide, wide, wide, wide,
            part, part, block, block, block, block, block,
            block, block, block, block, block, block,
            pltpu.VMEM((2, 1, 128), F32), pltpu.VMEM((plane, 1, 128), F32),
            pltpu.VMEM((max(nz - 1, 1), 1, 128), F32),
            pltpu.SemaphoreType.DMA((2,)), pltpu.SemaphoreType.DMA((18,)), pltpu.SemaphoreType.DMA((18,)),
            pltpu.SemaphoreType.DMA((peers,)), pltpu.SemaphoreType.DMA((peers,)),
            pltpu.SemaphoreType.REGULAR((4,)),
        ],
        compiler_params=pltpu.CompilerParams(
            collective_id=0, has_side_effects=True, vmem_limit_bytes=48 * 1024 * 1024
        ),
        name="siglip",
    )(log_scale, bias, in_hbm(image_embed), in_hbm(text_embed))
    return pl.pallas_call(
        write,
        out_shape=(
            jax.ShapeDtypeStruct((1,), F32),
            jax.ShapeDtypeStruct((rows, width), F32),
            jax.ShapeDtypeStruct((rows, width), F32),
        ),
        in_specs=[vmem, vmem, vmem],
        out_specs=(smem, hbm, hbm),
        scratch_shapes=[pltpu.SemaphoreType.DMA((2,))],
        compiler_params=pltpu.CompilerParams(vmem_limit_bytes=2 * 1024 * 1024),
        name="write",
    )(loss_row, img_grad, txt_grad)


def solution(mesh):
    split = Mesh(mesh.devices.reshape(16, 2, 2, 4, 2), AXES)
    rows = P(AXES, None)
    return jax.shard_map(
        local, mesh=split, in_specs=(rows, rows, P(), P()), out_specs=(P(), rows, rows), check_vma=False
    )
```

```python
import itertools

import jax
import jax.numpy as jnp
from jax import lax
from jax.experimental import pallas as pl
from jax.experimental.pallas import tpu as pltpu
from jax.sharding import Mesh
from jax.sharding import PartitionSpec as P

AXES = ("z", "yh", "yl", "x", "c")
MESH = pl.DeviceIdType.MESH
BF = jnp.bfloat16
F32 = jnp.float32
CHUNK = 384


def in_hbm(value):
    return pltpu.with_memory_space_constraint(value, pltpu.HBM)


def nt_dot(a, b):
    return lax.dot_general(a, b, (((1,), (1,)), ((), ())), preferred_element_type=F32)


def tn_dot(a, b):
    return lax.dot_general(a, b, (((0,), (0,)), ((), ())), preferred_element_type=F32)


def kernel(
    log_scale_ref, bias_ref, img_hbm, txt_hbm,
    loss_ref, img_grad, txt_grad,
    img_x, txt_x, img_inv, txt_inv, img_all, txt_all, logit, weight,
    own_p, hold_p, own_q, hold_q,
    out_right, out_left, out_opp, out_sib, out_diag, out_comb, out_part,
    way_x, fin_left, fin_right, way_t, fin_sib, fin_part,
    loss_out, loss_in1, loss_in3,
    load_sem, send_sem, recv_sem, lsend_sem, lrecv_sem, near_sem,
):
    rows, width = img_x.shape
    half = rows // 2
    nz, nyh, nx = lax.axis_size("z"), lax.axis_size("yh"), lax.axis_size("x")
    ny = 2 * nyh
    z, yh, yl = lax.axis_index("z"), lax.axis_index("yh"), lax.axis_index("yl")
    x, c = lax.axis_index("x"), lax.axis_index("c")
    y = yh * 2 + yl

    def at_x(step, core=0):
        return {"x": lax.rem(x + step, nx), "c": lax.rem(c + core, 2)}

    def at_y(step):
        there = lax.rem(y + step, ny)
        return {"yh": there // 2, "yl": lax.rem(there, 2)}

    def at_z(step):
        return {"z": lax.rem(z + step, nz)}

    right, left, sibling = at_x(1), at_x(nx - 1), at_x(0, 1)
    partner = {"yl": 1 - yl}

    load_img = pltpu.make_async_copy(img_hbm, img_x, load_sem.at[0])
    load_txt = pltpu.make_async_copy(txt_hbm, txt_x, load_sem.at[1])
    load_img.start()
    load_txt.start()

    near = [right, left, sibling, at_y(1), at_y(ny - 1)]
    barrier = pltpu.get_barrier_semaphore()

    def signal(semaphore, peers):
        for peer in peers:
            pl.semaphore_signal(semaphore, inc=1, device_id=peer, device_id_type=MESH)

    def signal_if(condition, semaphore, peers):
        @pl.when(condition)
        def _():
            signal(semaphore, peers)

    first_plane = z == 0
    later_plane = jnp.logical_not(first_plane)
    others = [at_z(step) for step in range(1, nz)]
    signal(barrier, near)
    signal_if(first_plane, barrier, others)

    def send(index, source, target, peer):
        copy = pltpu.make_async_remote_copy(
            src_ref=source, dst_ref=target, send_sem=send_sem.at[index], recv_sem=recv_sem.at[index],
            device_id=peer, device_id_type=MESH,
        )
        copy.start()
        return copy

    def normalize(values, inverse, packed):
        step = 32
        for start in range(0, rows, step):
            part = values[start : start + step, :]
            inv = lax.rsqrt(jnp.sum(part * part, axis=1, keepdims=True) + 1e-06)
            inverse[start : start + step, :] = inv
            packed[start : start + step, :] = (part * inv).astype(BF)

    a, b = pl.ds(0, half), pl.ds(half, half)

    def slot(index, offset=0, size=None):
        return pl.ds(index * rows + offset, rows if size is None else size)

    load_img.wait()
    normalize(img_x, img_inv, img_all)
    pl.semaphore_wait(barrier, len(near) + jnp.where(first_plane, 0, 1))
    right_a = send(0, img_all.at[a], img_all.at[slot(1, 0, half)], right)
    left_b = send(2, img_all.at[b], img_all.at[slot(2, half, half)], left)
    right_b = send(1, img_all.at[b], img_all.at[slot(1, half, half)], right)
    left_a = send(3, img_all.at[a], img_all.at[slot(2, 0, half)], left)
    load_txt.wait()
    normalize(txt_x, txt_inv, txt_all)
    txt_part = send(7, txt_all.at[slot(0)], txt_all.at[slot(2)], partner)
    txt_sib = send(6, txt_all.at[slot(0)], txt_all.at[slot(1)], sibling)

    def round_of(index, peers):
        signal(near_sem.at[index], peers)

    round_of(0, near)
    signal_if(later_plane, near_sem.at[3], [{"z": 0}])

    right_a.wait_recv()
    pass_right = send(4, img_all.at[slot(1, 0, half)], img_all.at[slot(3, 0, half)], right)
    left_b.wait_recv()
    pass_left = send(5, img_all.at[slot(2, half, half)], img_all.at[slot(3, half, half)], left)
    txt_part.wait_recv()
    txt_diag = send(8, txt_all.at[slot(2)], txt_all.at[slot(3)], sibling)
    pl.semaphore_wait(near_sem.at[0], len(near))
    round_of(1, [at_x(2), at_y(2), sibling])

    log_scale = jnp.full((1, 4 * rows), log_scale_ref[0], F32)
    scale = jnp.exp(log_scale)
    offset = jnp.full((1, 4 * rows), bias_ref[0], F32)

    def diagonal(shape):
        return lax.broadcasted_iota(jnp.int32, shape, 0) == lax.broadcasted_iota(jnp.int32, shape, 1)

    def logits_of(index):
        logits = scale * nt_dot(img_all[slot(index), :], txt_all[...]) + offset
        logit[slot(index), :] = logits

    def loss_of(index):
        logits = logit[slot(index), :]
        flip = jnp.maximum(logits, 0.0)
        if index == 0:
            flip = jnp.where(diagonal(logits.shape), jnp.maximum(-logits, 0.0), flip)
        terms = flip + jnp.log1p(jnp.exp(-jnp.abs(logits)))
        return jnp.sum(terms.reshape(rows // 8, 8, 4 * rows), axis=0)

    def weights(index):
        logits = logit[slot(index), :]
        small = jnp.exp(-jnp.abs(logits))
        inv = 1.0 / (1.0 + small)
        value = jnp.where(logits >= 0, 1.0, small) * inv
        if index == 0:
            value = jnp.where(diagonal(value.shape), -jnp.where(logits >= 0, small, 1.0) * inv, value)
        weight[slot(index), :] = value.astype(BF)

    def img_term(index, start):
        return jnp.dot(weight[slot(index), :], txt_all[:, start : start + CHUNK], preferred_element_type=F32)

    def txt_term(index, start):
        block = weight[:, index * rows : (index + 1) * rows]
        return tn_dot(block, img_all[:, start : start + CHUNK])

    chunks = [(start, slice(start, start + CHUNK)) for start in range(0, width, CHUNK)]

    txt_sib.wait_recv()
    txt_diag.wait_recv()
    logits_of(0)
    total = loss_of(0)
    weights(0)
    right_b.wait_recv()
    left_a.wait_recv()
    for index in (1, 2):
        logits_of(index)
        total = total + loss_of(index)
        weights(index)
    pl.semaphore_wait(near_sem.at[1], 3)
    round_of(2, [sibling])
    pass_right.wait_recv()
    pass_left.wait_recv()
    logits_of(3)
    total = jnp.sum(total + loss_of(3), axis=0, keepdims=True)
    total = sum(total[:, k * rows : (k + 1) * rows] for k in range(4))

    def messages(base, stage, inbox, peers):
        return [
            pltpu.make_async_remote_copy(
                src_ref=loss_out.at[stage], dst_ref=inbox.at[k], send_sem=lsend_sem.at[base + k],
                recv_sem=lrecv_sem.at[base + k], device_id=peer, device_id_type=MESH,
            )
            for k, peer in enumerate(peers)
        ]

    def spread(value, stage, copies):
        loss_out[stage] = value
        for copy in reversed(copies):
            copy.start()

    def gather(stage, copies, inbox):
        value = loss_out[stage]
        for k, copy in enumerate(copies):
            copy.wait_recv()
            value = value + inbox[k]
        return value

    def hops(step):
        dy, dx, dc = step
        return min(dy, ny - dy) + min(dx, nx - dx) + dc / 2

    plane = [
        {**at_x(dx, dc), **at_y(dy)}
        for dy, dx, dc in sorted(itertools.product(range(ny), range(nx), range(2)), key=hops)[1:]
    ]
    along = sorted(range(1, nz), key=lambda step: min(step, nz - step))
    first = messages(0, 0, loss_in1, plane)
    third = messages(len(plane), 1, loss_in3, [at_z(step) for step in along])
    pl.semaphore_wait(near_sem.at[2], 1)
    spread(total, 0, first)
    weights(3)
    for start, cols in chunks:
        term = img_term(2, start)
        hold_p[0:half, cols] = term[0:half]
        out_right[:, cols] = term[half:].astype(BF)
    to_right = send(11, out_right, fin_left.at[b], right)
    for start, cols in chunks:
        term = img_term(1, start)
        hold_p[half:, cols] = term[half:]
        out_left[:, cols] = term[0:half].astype(BF)
    to_left = send(12, out_left, fin_right.at[a], left)
    for start, cols in chunks:
        own_p[:, cols] = img_term(0, start)

    for start, cols in chunks:
        out_opp[:, cols] = img_term(3, start).astype(BF)
    opp_right = send(9, out_opp.at[a], way_x.at[a], right)
    opp_left = send(10, out_opp.at[b], way_x.at[b], left)
    for start, cols in chunks:
        out_diag[:, cols] = txt_term(3, start).astype(BF)
    diag = send(15, out_diag, way_t, sibling)
    for start, cols in chunks:
        out_sib[:, cols] = txt_term(1, start).astype(BF)
    sib = send(16, out_sib, fin_sib, sibling)
    for start, cols in chunks:
        hold_q[:, cols] = txt_term(2, start)
    for start, cols in chunks:
        own_q[:, cols] = txt_term(0, start)

    diag.wait_recv()
    for start, cols in chunks:
        out_part[:, cols] = (hold_q[:, cols] + way_t[:, cols].astype(F32)).astype(BF)
    part = send(17, out_part, fin_part, partner)

    @pl.when(first_plane)
    def _():
        if nz > 1:
            pl.semaphore_wait(near_sem.at[3], nz - 1)
            signal(near_sem.at[4], others)

    total = gather(0, first, loss_in1)

    @pl.when(later_plane)
    def _():
        pl.semaphore_wait(near_sem.at[4], 1)

    spread(total, 1, third)

    opp_right.wait_recv()
    out_comb[a] = (hold_p[a] + way_x[a].astype(F32)).astype(BF)
    comb_right = send(13, out_comb.at[a], fin_left.at[a], right)
    opp_left.wait_recv()
    out_comb[b] = (hold_p[b] + way_x[b].astype(F32)).astype(BF)
    comb_left = send(14, out_comb.at[b], fin_right.at[b], left)

    scale = jnp.exp(jnp.full((1, width), log_scale_ref[0], F32))

    def back(own, one, two, values, inverse, target):
        step = 32
        for start in range(0, rows, step):
            r = slice(start, start + step)
            grad = scale * (own[r, :] + one[r, :].astype(F32) + two[r, :].astype(F32))
            inv = inverse[r, :]
            unit = values[r, :] * inv
            target[r, :] = inv * (grad - jnp.sum(grad * unit, axis=1, keepdims=True) * unit)

    to_right.wait_recv()
    to_left.wait_recv()
    sib.wait_recv()
    part.wait_recv()
    back(own_q, fin_sib, fin_part, txt_x, txt_inv, txt_grad)
    comb_right.wait_recv()
    comb_left.wait_recv()
    back(own_p, fin_left, fin_right, img_x, img_inv, img_grad)

    total = gather(1, third, loss_in3)
    count = rows * 4 * nx * nyh * nz
    loss_ref[...] = total * (1.0 / count)

    for copy in (
        right_a, left_b, right_b, left_a, txt_part, txt_sib, pass_right, pass_left, txt_diag, to_right, to_left,
        opp_right, opp_left, diag, sib, part, comb_right, comb_left, *first, *third,
    ):
        copy.wait_send()


def write(loss_row, img_grad, txt_grad, loss_ref, img_out, txt_out, sems):
    copies = [
        pltpu.make_async_copy(img_grad, img_out, sems.at[0]),
        pltpu.make_async_copy(txt_grad, txt_out, sems.at[1]),
    ]
    for copy in copies:
        copy.start()
    loss_ref[0] = jnp.sum(loss_row[...])
    for copy in copies:
        copy.wait()


def local(image_embed, text_embed, log_scale, bias):
    rows, width = image_embed.shape
    half = rows // 2
    nx, ny, nz = lax.axis_size("x"), 2 * lax.axis_size("yh"), lax.axis_size("z")
    plane = 2 * nx * ny - 1
    peers = plane + nz - 1
    smem = pl.BlockSpec(memory_space=pltpu.SMEM)
    hbm = pl.BlockSpec(memory_space=pltpu.HBM)
    vmem = pl.BlockSpec(memory_space=pltpu.VMEM)
    block = pltpu.VMEM((rows, width), BF)
    wide = pltpu.VMEM((rows, width), F32)
    part = pltpu.VMEM((half, width), BF)
    column = pltpu.VMEM((rows, 1), F32)
    loss_row, img_grad, txt_grad = pl.pallas_call(
        kernel,
        out_shape=(
            jax.ShapeDtypeStruct((1, 128), F32),
            jax.ShapeDtypeStruct((rows, width), F32),
            jax.ShapeDtypeStruct((rows, width), F32),
        ),
        in_specs=[smem, smem, hbm, hbm],
        out_specs=(vmem, vmem, vmem),
        scratch_shapes=[
            wide, wide, column, column,
            pltpu.VMEM((4 * rows, width), BF), pltpu.VMEM((4 * rows, width), BF),
            pltpu.VMEM((4 * rows, 4 * rows), F32), pltpu.VMEM((4 * rows, 4 * rows), BF),
            wide, wide, wide, wide,
            part, part, block, block, block, block, block,
            block, block, block, block, block, block,
            pltpu.VMEM((2, 1, 128), F32), pltpu.VMEM((plane, 1, 128), F32),
            pltpu.VMEM((max(nz - 1, 1), 1, 128), F32),
            pltpu.SemaphoreType.DMA((2,)), pltpu.SemaphoreType.DMA((18,)), pltpu.SemaphoreType.DMA((18,)),
            pltpu.SemaphoreType.DMA((peers,)), pltpu.SemaphoreType.DMA((peers,)),
            pltpu.SemaphoreType.REGULAR((5,)),
        ],
        compiler_params=pltpu.CompilerParams(
            collective_id=0, has_side_effects=True, vmem_limit_bytes=48 * 1024 * 1024
        ),
        name="siglip",
    )(log_scale, bias, in_hbm(image_embed), in_hbm(text_embed))
    return pl.pallas_call(
        write,
        out_shape=(
            jax.ShapeDtypeStruct((1,), F32),
            jax.ShapeDtypeStruct((rows, width), F32),
            jax.ShapeDtypeStruct((rows, width), F32),
        ),
        in_specs=[vmem, vmem, vmem],
        out_specs=(smem, hbm, hbm),
        scratch_shapes=[pltpu.SemaphoreType.DMA((2,))],
        compiler_params=pltpu.CompilerParams(vmem_limit_bytes=2 * 1024 * 1024),
        name="write",
    )(loss_row, img_grad, txt_grad)


def solution(mesh):
    split = Mesh(mesh.devices.reshape(16, 2, 2, 4, 2), AXES)
    rows = P(AXES, None)
    return jax.shard_map(
        local, mesh=split, in_specs=(rows, rows, P(), P()), out_specs=(P(), rows, rows), check_vma=False
    )
```
